32 devices in a mesh: gx: 4 (over z), gy: 4 (over x, core), col: 2 (over y).
Axes of the slice: x: 2, y: 2, z: 4, core: 2. Of those that a mesh axis runs over, the one named last changes fastest.
Arguments:
- fields: bfloat16 [2, 128, 128, 32, 128], P('col', 'gx', 'gy'), may hold values from -6 to 6
- spectral: bfloat16 [1, 16, 16, 2, 32, 32, 16], P(None, 'gx', 'gy', None, None, 'col'), may hold values from -0.75 to 0.75
- skip_weight: bfloat16 [1, 32, 32], replicated, may hold values from -1 to 1
- skip_bias: float32 [1, 32], replicated, may hold values from -3 to 3
- norm_gain: float32 [1, 32], replicated, may hold values from 0.5 to 1.5
- norm_shift: float32 [1, 32], replicated, may hold values from -3 to 3
Outputs:
- activations: bfloat16 [2, 128, 128, 32, 128], P('col', 'gx', 'gy')
The draws below stay inside these ranges and needn't reach their ends.
All inputs are finite; a program needn't handle non-finite values.
Results may differ from the reference program's by a relative error of at most 0.012.
Values may be sent and summed in bfloat16 or wider, within the bound.
A program may use at most 128 MiB of HBM per device.

```python
import math
import jax
import jax.numpy as jnp
from jax import lax

X = 128
Y = 128
Z = 128
C = 32
MX = 16
MY = 16
MZ = 16
LAYERS = 1
SAMPLES = 2


def block_levels(own_key, shape, split, low, largest):
    def one(dim, shards_of):
        draws = jax.random.uniform(jax.random.fold_in(jax.random.fold_in(own_key, 6), dim), (shards_of,), jnp.float32, low / len(split), largest / len(split))
        return jnp.repeat(jnp.exp(draws), shape[dim] // shards_of).reshape((-1,) + (1,) * (len(shape) - dim - 1))

    level = one(*split[0])
    for cut in split[1:]:
        level = level * one(*cut)
    return level


def scatter_about(stream_key, dims, scale, bound, split=(), kind=jnp.bfloat16):
    gain = block_levels(stream_key, dims, split, -0.22, 0.18) if split else 1.0
    array = jax.random.normal(stream_key, dims, jnp.float32) * scale * gain
    return jnp.minimum(jnp.maximum(array, -bound), bound).astype(kind)


def setup_inputs(seed: int = 0) -> dict:
    keys = jax.random.split(jax.random.key(seed), 7)
    fields = scatter_about(keys[0], (SAMPLES, X, Y, C, Z), 1.0, 6.0, ((0, 2), (1, 4), (2, 4)))
    spectral = scatter_about(keys[1], (LAYERS, MX, MY, 2, C, C, MZ), (2 * C) ** -0.5, 0.75, ((1, 4), (2, 4), (5, 2)))
    skip_weight = scatter_about(keys[2], (LAYERS, C, C), C ** -0.5, 1.0)
    skip_bias = scatter_about(keys[3], (LAYERS, C), 0.5, 3.0, (), jnp.float32)
    norm_gain = jnp.clip(jax.random.uniform(keys[4], (LAYERS, C), jnp.float32, 0.5, 1.5), 0.5, 1.5)
    norm_shift = scatter_about(keys[5], (LAYERS, C), 0.5, 3.0, (), jnp.float32)
    return dict(fields=fields, spectral=spectral, skip_weight=skip_weight, skip_bias=skip_bias, norm_gain=norm_gain, norm_shift=norm_shift)


norm_eps = 1e-05

def signed_freqs(count):
    index = jnp.arange(count, dtype=jnp.int32)
    return jnp.where(index < count // 2, index, index - count)

def angles(positions, frequency, length):
    turn_count = positions[:, None] * frequency[None, :] % length
    return turn_count.astype(jnp.float32) * (2.0 * math.pi / length)

def forward_table(positions, frequency, length, factor):
    phase_angle = angles(positions, frequency, length)
    cosine = jnp.cos(phase_angle) * factor
    sine_part = jnp.sin(phase_angle) * factor
    from_real = jnp.stack([cosine, -sine_part], axis=-1)
    from_imag = jnp.stack([sine_part, cosine], axis=-1)
    return jnp.stack([from_real, from_imag], axis=1)

def inverse_table(frequency, positions, length):
    phase_angle = angles(positions, frequency, length).T
    cosine = jnp.cos(phase_angle)
    sine_part = jnp.sin(phase_angle)
    from_real = jnp.stack([cosine, sine_part], axis=-1)
    from_imag = jnp.stack([-sine_part, cosine], axis=-1)
    return jnp.stack([from_real, from_imag], axis=1)

def depth_tables(length, count):
    frequency = jnp.arange(count, dtype=jnp.int32)
    phase_angle = angles(jnp.arange(length, dtype=jnp.int32), frequency, length)
    forward = jnp.concatenate([jnp.cos(phase_angle), -jnp.sin(phase_angle)], axis=1)
    backward = jnp.concatenate([jnp.cos(phase_angle).T, -jnp.sin(phase_angle).T], axis=0)
    return (forward.astype(jnp.bfloat16), backward.astype(jnp.bfloat16))

def mix_modes(spectrum, weight):

    def contract(left, right):
        return jnp.einsum('abcz,abcdz->abdz', left, right, preferred_element_type=jnp.float32, precision=lax.Precision.HIGHEST)
    real_in = spectrum[:, :, :, 0]
    imag_in = spectrum[:, :, :, 1]
    real_weight = weight[:, :, 0]
    imag_weight = weight[:, :, 1]
    real_out = contract(real_in, real_weight) - contract(imag_in, imag_weight)
    imag_out = contract(real_in, imag_weight) + contract(imag_in, real_weight)
    return jnp.stack([real_out, imag_out], axis=3)

def finish(spectral_part, skip_part, offset, scaling, shift_term):
    pre_norm = spectral_part + skip_part + offset[:, None]
    centre = lax.optimization_barrier(jnp.mean(pre_norm, axis=2, keepdims=True))
    spread = lax.optimization_barrier(jnp.mean(jnp.square(pre_norm - centre), axis=2, keepdims=True))
    normed = (pre_norm - centre) * lax.rsqrt(spread + norm_eps) * scaling[:, None] + shift_term[:, None]
    return jax.nn.gelu(normed, approximate=False).astype(jnp.bfloat16)

def sample_layers(sample, spectral, skip_weight, skip_bias, norm_gain, norm_shift):
    highest = lax.Precision.HIGHEST
    depth_forward, depth_backward = depth_tables(Z, MZ)
    first_cells = jnp.arange(X, dtype=jnp.int32)
    second_cells = jnp.arange(Y, dtype=jnp.int32)
    second_forward = forward_table(second_cells, signed_freqs(MY), Y, 1.0).astype(jnp.bfloat16)
    first_forward = forward_table(first_cells, signed_freqs(MX), X, 1.0 / math.sqrt(X * Y * Z))
    first_inverse = inverse_table(signed_freqs(MX), first_cells, X).astype(jnp.bfloat16)
    second_inverse = inverse_table(signed_freqs(MY), second_cells, Y)
    inverse_scale = 1.0 / math.sqrt(MX * MY * MZ)
    hidden = sample
    for layer_index in range(LAYERS):
        amplitude = jnp.dot(hidden.reshape(-1, Z).astype(jnp.float32), depth_forward.astype(jnp.float32), precision=highest)
        amplitude = amplitude.astype(jnp.bfloat16).reshape(X, Y, C, 2, MZ)
        along_second = jnp.einsum('xycrz,yrks->xkcsz', amplitude.astype(jnp.float32), second_forward.astype(jnp.float32), precision=highest)
        spectrum_sum = jnp.einsum('xkcsz,xsjt->jkctz', along_second, first_forward, precision=highest)
        spectrum = spectrum_sum.astype(jnp.bfloat16)
        mixed_modes = mix_modes(spectrum.astype(jnp.float32), spectral[layer_index].astype(jnp.float32)).astype(jnp.bfloat16)
        rows_first = jnp.einsum('jkcsz,jsxt->xkctz', mixed_modes.astype(jnp.float32), first_inverse.astype(jnp.float32), precision=highest)
        rows_both = jnp.einsum('xkcsz,ksyt->xyctz', rows_first, second_inverse, precision=highest).astype(jnp.bfloat16)
        spectral_part = jnp.dot(rows_both.reshape(-1, 2 * MZ).astype(jnp.float32), depth_backward.astype(jnp.float32), precision=highest)
        spectral_part = spectral_part.reshape(X, Y, C, Z) * inverse_scale
        skip_part = jnp.einsum('oc,xycz->xyoz', skip_weight[layer_index].astype(jnp.float32), hidden.astype(jnp.float32), precision=highest)
        hidden = finish(spectral_part, skip_part, skip_bias[layer_index], norm_gain[layer_index], norm_shift[layer_index])
    return hidden

def reference(fields, spectral, skip_weight, skip_bias, norm_gain, norm_shift):

    def per_sample(sample):
        return sample_layers(sample, spectral, skip_weight, skip_bias, norm_gain, norm_shift)
    return lax.map(per_sample, fields)
```

```python
import functools
import math

import jax
import jax.numpy as jnp
import numpy as np
from jax import lax
from jax.experimental import pallas as pl
from jax.experimental.pallas import tpu as pltpu
from jax.sharding import PartitionSpec as P

norm_eps = 1e-05
BF = jnp.bfloat16
F32 = jnp.float32
MESH = pl.DeviceIdType.MESH


def signed(count):
    index = np.arange(count)
    return np.where(index < count // 2, index, index - count)


def cos_sin(positions, frequency, length):
    turns = (positions[:, None] * frequency[None, :]) % length
    phase = turns * (2.0 * math.pi / length)
    return np.cos(phase), np.sin(phase)


def log2(n):
    assert n & (n - 1) == 0
    return n.bit_length() - 1


def div(i, n):
    return lax.shift_right_logical(i, jnp.int32(log2(n)))


def mod(i, n):
    return lax.bitwise_and(i, jnp.int32(n - 1))


def iota(shape, dim):
    return lax.broadcasted_iota(jnp.int32, shape, dim)


def dot(a, b):
    return jnp.dot(a, b, preferred_element_type=F32)


def expand(table, rows, cols, row_of, col_of, row_key, col_key, first_row=0, less=0.0):
    r, c = table.shape
    left = (row_of(iota((rows, r), 0) + first_row) == iota((rows, r), 1)).astype(F32).astype(BF)
    right = (col_of(iota((c, cols), 1)) == iota((c, cols), 0)).astype(F32).astype(BF)
    full = dot(dot(left, table).astype(BF), right)
    keep = row_key(iota((rows, cols), 0) + first_row) == col_key(iota((rows, cols), 1))
    return (full * jnp.where(keep, 1.0 - less, -less)).astype(BF)


def kron_eye(table, n, store, chunk=256):
    rows, cols = table.shape[0] * n, table.shape[1] * n
    chunk = min(chunk, rows)
    for first in range(0, rows, chunk):
        store(
            first,
            expand(
                table, chunk, cols,
                lambda i: div(i, n), lambda j: div(j, n),
                lambda i: mod(i, n), lambda j: mod(j, n), first,
            ),
        )


def front_kernel(
    sizes,
    fields_ref, spectral_ref, depth_ref, tyf_ref, txf_ref, txi_ref, tyi_ref,
    out_ref,
    ky_ref, total_ref, send_ref, recv_ref, spec_ref, mix_ref, modes_ref, gx_ref, hy_ref, w_ref,
    wsem, send1, recv1, send2, recv2, send3, recv3,
):
    n_gx, n_gy, n_col, xl, yl, C, MY, MZ, kxl, kyl, dl, G, steps = sizes
    nxy, N = n_gx * n_gy, n_gx * n_gy * n_col
    L = 2 * kxl * MZ
    step = pl.program_id(0)
    gx, gy, col = lax.axis_index("gx"), lax.axis_index("gy"), lax.axis_index("col")
    place = gx * n_gy + gy
    me = place * n_col + col

    def target(linear):
        return (linear // (n_gy * n_col), (linear // n_col) % n_gy, linear % n_col)

    weights_copy = pltpu.make_async_copy(spectral_ref, w_ref, wsem)

    @pl.when(step == 0)
    def _():
        barrier = pltpu.get_barrier_semaphore()

        def greet(i, carry):
            px, py, pc = target((me + i) % N)
            pl.semaphore_signal(
                barrier, inc=1, device_id={"gx": px, "gy": py, "col": pc}, device_id_type=MESH
            )
            return carry

        lax.fori_loop(1, N, greet, 0)
        weights_copy.start()

        def put(first, value):
            ky_ref[pl.ds(first, value.shape[0]), :] = value

        kron_eye(tyf_ref[gy], C, put)
        total_ref[...] = jnp.zeros_like(total_ref)

    lhs = jnp.concatenate([fields_ref[g] for g in range(G)], axis=-1)
    amplitude = dot(lhs, depth_ref[...]).astype(BF)
    turned = dot(ky_ref[...], amplitude).astype(BF)
    half = MY * C
    acc = None
    for cs in range(2):
        parts = []
        kron_eye(txf_ref[gx, step, cs], MZ, lambda f, v: parts.append(v))
        kx = parts[0] if len(parts) == 1 else jnp.concatenate(parts, axis=0)
        term = dot(turned[cs * half:(cs + 1) * half], kx)
        acc = term if acc is None else acc + term
    total_ref[...] += acc

    @pl.when(step == steps - 1)
    def _():
        rows = kyl * C
        for b in range(n_gx):
            block = total_ref[:, b * L:(b + 1) * L].astype(BF)
            for q in range(n_gy):
                send_ref[b, q] = block[q * rows:(q + 1) * rows]
        pl.semaphore_wait(pltpu.get_barrier_semaphore(), N - 1)

        def scatter(i):
            other = (place + i) % nxy
            return pltpu.make_async_remote_copy(
                src_ref=send_ref.at[other // n_gy, other % n_gy], dst_ref=recv_ref.at[i],
                send_sem=send1.at[i], recv_sem=recv1.at[i],
                device_id={"gx": other // n_gy, "gy": other % n_gy}, device_id_type=MESH,
            )

        def loop(low, high, body):
            def go(i, carry):
                body(i)
                return carry
            lax.fori_loop(low, high, go, 0)

        loop(1, nxy, lambda i: scatter(i).start())

        for cs in range(2):
            def put(first, value, cs=cs):
                gx_ref[cs, pl.ds(first, value.shape[0]), :] = value
            kron_eye(txi_ref[gx, cs], MZ, put)
        chunk = min(256, yl * C)
        for first in range(0, yl * C, chunk):
            hy_ref[pl.ds(first, chunk), :] = expand(
                tyi_ref[gy], chunk, 2 * MY * C,
                lambda i: div(i, C),
                lambda j: div(j, n_col * kyl * dl) * kyl + mod(div(j, dl), kyl),
                lambda i: mod(i, C),
                lambda j: mod(div(j, kyl * dl), n_col) * dl + mod(j, dl),
                first, 1.0 / C,
            )
        weights_copy.wait()

        sum_ = send_ref[gx, gy].astype(F32)
        for i in range(1, nxy):
            scatter(i).wait_recv()
            sum_ = sum_ + recv_ref[i].astype(F32)
        spec_ref[col] = sum_.astype(BF)

        def share(i):
            return pltpu.make_async_remote_copy(
                src_ref=spec_ref.at[col], dst_ref=spec_ref.at[col],
                send_sem=send2.at[i], recv_sem=recv2.at[i],
                device_id={"col": (col + i) % n_col}, device_id_type=MESH,
            )

        for i in range(1, n_col):
            share(i).start()
        packed = []
        for k in range(kyl):
            real = jnp.concatenate([w_ref[j, k, 0].astype(F32) for j in range(kxl)], axis=-1)
            imag = jnp.concatenate([w_ref[j, k, 1].astype(F32) for j in range(kxl)], axis=-1)
            packed.append((
                jnp.concatenate([real, imag], axis=-1), jnp.concatenate([-imag, real], axis=-1)
            ))
        for i in range(1, n_col):
            share(i).wait_recv()
        for s in range(n_col):
            spec = spec_ref[s].astype(F32)
            re, im = spec[:, :L // 2], spec[:, L // 2:]
            re = jnp.concatenate([re, re], axis=-1)
            im = jnp.concatenate([im, im], axis=-1)
            for k in range(kyl):
                wa, wb = packed[k]
                mixed = jnp.sum(
                    re[k * C:(k + 1) * C][:, None, :] * wa + im[k * C:(k + 1) * C][:, None, :] * wb,
                    axis=0,
                )
                mix_ref[s, k * dl:(k + 1) * dl] = mixed.astype(BF)
        modes_ref[gx, gy, col] = mix_ref[col]

        def gather(i):
            px, py, pc = target((me + i) % N)
            return pltpu.make_async_remote_copy(
                src_ref=mix_ref.at[pc], dst_ref=modes_ref.at[gx, gy, col],
                send_sem=send3.at[i], recv_sem=recv3.at[i],
                device_id={"gx": px, "gy": py, "col": pc}, device_id_type=MESH,
            )

        loop(1, N, lambda i: gather(i).start())
        loop(1, nxy, lambda i: scatter(i).wait_send())
        for i in range(1, n_col):
            share(i).wait_send()
        loop(1, N, lambda i: gather(i).wait_recv())
        full = jnp.concatenate(
            [modes_ref[b].reshape(MY * C, L) for b in range(n_gx)], axis=-1
        )
        first_inverse = jnp.concatenate(
            [dot(full, gx_ref[cs]).astype(BF) for cs in range(2)], axis=0
        )
        out_ref[...] = dot(hy_ref[...], first_inverse).astype(BF)
        loop(1, N, lambda i: gather(i).wait_send())


def back_kernel(
    sizes, rows_ref, fields_ref, depth_ref, skip_ref, bias_ref, gain_ref, shift_ref, out_ref, wbd_ref
):
    G, C, MZ, Z, rows, tile = sizes

    @pl.when(pl.program_id(0) == 0)
    def _():
        weight = skip_ref[...].astype(F32)
        weight = (weight - jnp.mean(weight, axis=0, keepdims=True)).astype(BF)
        wbd_ref[...] = expand(
            weight, tile, tile,
            lambda i: mod(i, C), lambda j: mod(j, C), lambda i: div(i, C), lambda j: div(j, C),
        )

    bias = bias_ref[...]
    bias = (bias - jnp.mean(bias, axis=0, keepdims=True))[None]
    gain = gain_ref[...][None]
    shift = shift_ref[...][None]
    for first in range(0, rows, tile):
        for x in range(0, G, 2):
            hidden = jnp.concatenate(
                [fields_ref[x + k, first:first + tile] for k in range(2)], axis=-1
            )
            pre = dot(wbd_ref[...], hidden) + dot(
                rows_ref[first:first + tile, x * 2 * MZ:(x + 2) * 2 * MZ], depth_ref[...]
            )
            pre = pre.reshape(tile // C, C, 2 * Z) + bias
            spread = jnp.mean(pre * pre, axis=1, keepdims=True)
            normed = pre * (lax.rsqrt(spread + norm_eps) * gain) + shift
            value = (0.5 * normed) * (1.0 + lax.erf(normed * (0.5 ** 0.5)))
            value = value.astype(BF).reshape(tile, 2 * Z)
            for k in range(2):
                out_ref[x + k, first:first + tile] = value[:, k * Z:(k + 1) * Z]


def build(mesh):
    n_gx, n_gy, n_col = (mesh.shape[a] for a in ("gx", "gy", "col"))

    def local(fields, spectral, skip_weight, skip_bias, norm_gain, norm_shift):
        hidden = fields[0]
        xl, yl, C, Z = hidden.shape
        weights = spectral[0]
        kxl, kyl, _, _, dl, MZ = weights.shape
        X, Y, MX, MY = xl * n_gx, yl * n_gy, kxl * n_gx, kyl * n_gy
        G = min(8, xl)
        steps = xl // G
        L = 2 * kxl * MZ
        N, nxy = n_gx * n_gy * n_col, n_gx * n_gy

        cz, sz = cos_sin(np.arange(Z), np.arange(MZ), Z)
        forward = np.concatenate([cz, -sz], axis=1)
        depth_forward = np.kron(np.eye(G), forward)
        backward = np.concatenate([cz.T, -sz.T], axis=0) / math.sqrt(MX * MY * MZ)
        depth_backward = np.kron(np.eye(2), backward)
        cy, sy = cos_sin(np.arange(Y), signed(MY), Y)
        tyf = np.stack([cy, sy]).reshape(2, n_gy, yl, MY).transpose(1, 0, 3, 2)
        tyf = tyf.reshape(n_gy, 2 * MY, yl)
        tyi = np.stack([cy, sy]).reshape(2, n_gy, yl, MY).transpose(1, 2, 0, 3)
        tyi = tyi.reshape(n_gy, yl, 2 * MY)
        cx, sx = cos_sin(np.arange(X), signed(MX), X)
        f = np.stack([
            np.stack([np.stack([cx, -sx], 1), np.stack([sx, cx], 1)], 1),
            np.stack([np.stack([-sx, -cx], 1), np.stack([cx, -sx], 1)], 1),
        ]) / math.sqrt(X * Y * Z)
        f = f.reshape(2, n_gx, steps, G, 2, 2, n_gx, kxl).transpose(1, 2, 0, 3, 4, 6, 5, 7)
        txf = f.reshape(n_gx, steps, 2, 2 * G, 2 * MX)
        b = np.stack([
            np.stack([np.stack([cx, sx]), np.stack([-sx, cx])]),
            np.stack([np.stack([-sx, cx]), np.stack([-cx, -sx])]),
        ])
        b = b.reshape(2, 2, 2, n_gx, xl, n_gx, kxl).transpose(3, 0, 5, 1, 6, 4, 2)
        txi = b.reshape(n_gx, 2, 2 * MX, 2 * xl)
        const = lambda a: jnp.asarray(a.astype(np.float32)).astype(BF)

        cells = hidden.reshape(xl, yl * C, Z)
        whole = lambda shape: pl.BlockSpec(shape, lambda i: (0,) * len(shape))
        sizes = (n_gx, n_gy, n_col, xl, yl, C, MY, MZ, kxl, kyl, dl, G, steps)
        tables = [const(t) for t in (depth_forward, tyf, txf, txi, tyi)]
        rows_both = pl.pallas_call(
            functools.partial(front_kernel, sizes),
            grid=(steps,),
            out_shape=jax.ShapeDtypeStruct((yl * C, xl * 2 * MZ), BF),
            in_specs=[
                pl.BlockSpec((G, yl * C, Z), lambda i: (i, 0, 0)),
                pl.BlockSpec(memory_space=pl.ANY),
            ] + [whole(t.shape) for t in tables],
            out_specs=whole((yl * C, xl * 2 * MZ)),
            scratch_shapes=[
                pltpu.VMEM((2 * MY * C, yl * C), BF),
                pltpu.VMEM((MY * C, 2 * MX * MZ), F32),
                pltpu.VMEM((n_gx, n_gy, kyl * C, L), BF),
                pltpu.VMEM((nxy, kyl * C, L), BF),
                pltpu.VMEM((n_col, kyl * C, L), BF),
                pltpu.VMEM((n_col, kyl * dl, L), BF),
                pltpu.VMEM((n_gx, n_gy, n_col, kyl * dl, L), BF),
                pltpu.VMEM((2, 2 * MX * MZ, 2 * xl * MZ), BF),
                pltpu.VMEM((yl * C, 2 * MY * C), BF),
                pltpu.VMEM(weights.shape, BF),
                pltpu.SemaphoreType.DMA,
                pltpu.SemaphoreType.DMA((nxy,)),
                pltpu.SemaphoreType.DMA((nxy,)),
                pltpu.SemaphoreType.DMA((n_col,)),
                pltpu.SemaphoreType.DMA((n_col,)),
                pltpu.SemaphoreType.DMA((N,)),
                pltpu.SemaphoreType.DMA((N,)),
            ],
            compiler_params=pltpu.CompilerParams(
                collective_id=0, has_side_effects=True, vmem_limit_bytes=60 * 2**20,
                dimension_semantics=("arbitrary",),
            ),
            name="front",
        )(cells, weights, *tables)

        G2 = min(4, xl)
        rows = yl * C
        tile = min(256, rows)
        out = pl.pallas_call(
            functools.partial(back_kernel, (G2, C, MZ, Z, rows, tile)),
            grid=(xl // G2,),
            out_shape=jax.ShapeDtypeStruct(cells.shape, BF),
            in_specs=[
                pl.BlockSpec((rows, G2 * 2 * MZ), lambda i: (0, i)),
                pl.BlockSpec((G2, rows, Z), lambda i: (i, 0, 0)),
                whole((4 * MZ, 2 * Z)), whole((C, C)), whole((C, 1)), whole((C, 1)), whole((C, 1)),
            ],
            out_specs=pl.BlockSpec((G2, rows, Z), lambda i: (i, 0, 0)),
            scratch_shapes=[pltpu.VMEM((tile, tile), BF)],
            compiler_params=pltpu.CompilerParams(
                vmem_limit_bytes=40 * 2**20, dimension_semantics=("arbitrary",)
            ),
            name="back",
        )(
            rows_both, cells, const(depth_backward), skip_weight[0],
            skip_bias[0][:, None], norm_gain[0][:, None], norm_shift[0][:, None],
        )
        return out.reshape(1, xl, yl, C, Z)

    return local


def solution(mesh):
    placed = (
        P("col", "gx", "gy", None, None),
        P(None, "gx", "gy", None, None, "col", None),
        P(), P(), P(), P(),
    )
    return jax.shard_map(
        build(mesh), mesh=mesh, in_specs=placed,
        out_specs=P("col", "gx", "gy", None, None), check_vma=False,
    )
```

```python
import functools
import math

import jax
import jax.numpy as jnp
import numpy as np
from jax import lax
from jax.experimental import pallas as pl
from jax.experimental.pallas import tpu as pltpu
from jax.sharding import PartitionSpec as P

norm_eps = 1e-05
BF = jnp.bfloat16
F32 = jnp.float32
MESH = pl.DeviceIdType.MESH


def signed(count):
    index = np.arange(count)
    return np.where(index < count // 2, index, index - count)


def cos_sin(positions, frequency, length):
    turns = (positions[:, None] * frequency[None, :]) % length
    phase = turns * (2.0 * math.pi / length)
    return np.cos(phase), np.sin(phase)


def log2(n):
    assert n & (n - 1) == 0
    return n.bit_length() - 1


def div(i, n):
    return lax.shift_right_logical(i, jnp.int32(log2(n)))


def mod(i, n):
    return lax.bitwise_and(i, jnp.int32(n - 1))


def iota(shape, dim):
    return lax.broadcasted_iota(jnp.int32, shape, dim)


def dot(a, b):
    return jnp.dot(a, b, preferred_element_type=F32)


def expand(table, rows, cols, row_of, col_of, row_key, col_key, first_row=0):
    r, c = table.shape
    left = (row_of(iota((rows, r), 0) + first_row) == iota((rows, r), 1)).astype(F32).astype(BF)
    right = (col_of(iota((c, cols), 1)) == iota((c, cols), 0)).astype(F32).astype(BF)
    full = dot(dot(left, table).astype(BF), right)
    keep = row_key(iota((rows, cols), 0) + first_row) == col_key(iota((rows, cols), 1))
    return jnp.where(keep, full, 0.0).astype(BF)


def kron_eye(table, n, store, chunk=256):
    rows, cols = table.shape[0] * n, table.shape[1] * n
    chunk = min(chunk, rows)
    for first in range(0, rows, chunk):
        store(
            first,
            expand(
                table, chunk, cols,
                lambda i: div(i, n), lambda j: div(j, n),
                lambda i: mod(i, n), lambda j: mod(j, n), first,
            ),
        )


def front_kernel(
    sizes,
    fields_ref, spectral_ref, depth_ref, tyf_ref, txf_ref, txi_ref, tyi_ref,
    out_ref,
    ky_ref, kx_ref, total_ref, send_ref, recv_ref, spec_ref, mix_ref, modes_ref, gx_ref, hy_ref,
    cm_ref, w_ref, wa_ref, wb_ref,
    wsem, send1, recv1, send2, recv2, send3, recv3,
):
    n_gx, n_gy, n_col, xl, yl, C, MY, MZ, kxl, kyl, dl, G, steps, halves = sizes
    nxy, N = n_gx * n_gy, n_gx * n_gy * n_col
    L = 2 * kxl * MZ
    CH = C // halves
    per = n_col // halves
    half, step = pl.program_id(0), pl.program_id(1)
    gx, gy, col = lax.axis_index("gx"), lax.axis_index("gy"), lax.axis_index("col")
    place = gx * n_gy + gy
    me = place * n_col + col

    def target(linear):
        return (linear // (n_gy * n_col), (linear // n_col) % n_gy, linear % n_col)

    def loop(low, high, body):
        def go(i, carry):
            body(i)
            return carry
        lax.fori_loop(low, high, go, 0)

    weights_copy = pltpu.make_async_copy(spectral_ref, w_ref, wsem)

    @pl.when((half == 0) & (step == 0))
    def _():
        barrier = pltpu.get_barrier_semaphore()

        def greet(i):
            px, py, pc = target((me + i) % N)
            pl.semaphore_signal(
                barrier, inc=1, device_id={"gx": px, "gy": py, "col": pc}, device_id_type=MESH
            )

        loop(1, N, greet)
        weights_copy.start()

        def put(first, value):
            ky_ref[pl.ds(first, value.shape[0]), :] = value

        kron_eye(tyf_ref[gy], CH, put)

    @pl.when(half == 0)
    def _():
        for cs in range(2):
            def put(first, value, cs=cs):
                kx_ref[step, cs, pl.ds(first, value.shape[0]), :] = value
            kron_eye(txf_ref[gx, step, cs], MZ, put)

    lhs = jnp.concatenate(
        [fields_ref[g].reshape(yl * CH, fields_ref.shape[-1]) for g in range(G)], axis=-1
    )
    amplitude = dot(lhs, depth_ref[...]).astype(BF)
    turned = dot(ky_ref[...], amplitude).astype(BF)
    top = MY * CH
    term = dot(turned[:top], kx_ref[step, 0]) + dot(turned[top:], kx_ref[step, 1])

    @pl.when(step == 0)
    def _():
        total_ref[...] = term

    @pl.when(step > 0)
    def _():
        total_ref[...] += term

    def scatter(h, i):
        other = (place + i) % nxy
        return pltpu.make_async_remote_copy(
            src_ref=send_ref.at[h, other // n_gy, other % n_gy], dst_ref=recv_ref.at[h, i],
            send_sem=send1.at[h, i], recv_sem=recv1.at[h, i],
            device_id={"gx": other // n_gy, "gy": other % n_gy}, device_id_type=MESH,
        )

    @pl.when(step == steps - 1)
    def _():
        rows = kyl * CH
        for b in range(n_gx):
            block = total_ref[:, b * L:(b + 1) * L].astype(BF)
            for q in range(n_gy):
                send_ref[half, b, q] = block[q * rows:(q + 1) * rows]

        @pl.when(half == 0)
        def _():
            pl.semaphore_wait(pltpu.get_barrier_semaphore(), N - 1)

        loop(1, nxy, lambda i: scatter(half, i).start())

    @pl.when((half == halves - 1) & (step == steps - 1))
    def _():
        weights_copy.wait()
        eye = (iota((C, C), 0) == iota((C, C), 1)).astype(F32).astype(BF)
        turn = lambda a: lax.dot_general(
            eye, a, (((1,), (1,)), ((), ())), preferred_element_type=F32
        )
        for k in range(kyl):
            for d in range(dl):
                parts = [[w_ref[j, k, r, d] for j in range(kxl)] for r in range(2)]
                wa_ref[k, d] = turn(jnp.concatenate(parts[0] + parts[1], axis=0))
                wb_ref[k, d] = turn(jnp.concatenate(parts[1] + parts[0], axis=0))
        for cs in range(2):
            def put(first, value, cs=cs):
                gx_ref[cs, pl.ds(first, value.shape[0]), :] = value
            kron_eye(txi_ref[gx, cs], MZ, put)
        chunk = min(256, yl * CH)
        for first in range(0, yl * CH, chunk):
            hy_ref[pl.ds(first, chunk), :] = expand(
                tyi_ref[gy], chunk, 2 * MY * CH,
                lambda i: div(i, CH),
                lambda j: div(j, per * kyl * dl) * kyl + mod(div(j, dl), kyl),
                lambda i: mod(i, CH),
                lambda j: mod(div(j, kyl * dl), per) * dl + mod(j, dl),
                first,
            )
        shape = (MY * C, MY * C)
        i, j = iota(shape, 0), iota(shape, 1)
        in_half = mod(i, MY * CH)
        gy_i = div(in_half, per * kyl * dl)
        col_i = div(i, MY * CH) * per + mod(div(in_half, kyl * dl), per)
        source = (gy_i * n_col + col_i) * (kyl * dl) + mod(in_half, kyl * dl)
        same = (gy_i == div(j, n_col * kyl * dl)) & (mod(div(i, dl), kyl) == mod(div(j, dl), kyl))
        cm_ref[...] = (
            (source == j).astype(F32) - jnp.where(same, 1.0 / C, 0.0)
        ).astype(BF)

        def share(h, i):
            return pltpu.make_async_remote_copy(
                src_ref=spec_ref.at[col, h], dst_ref=spec_ref.at[col, h],
                send_sem=send2.at[h, i], recv_sem=recv2.at[h, i],
                device_id={"col": (col + i) % n_col}, device_id_type=MESH,
            )

        for h in range(halves):
            total = send_ref[h, gx, gy].astype(F32)
            for i in range(1, nxy):
                scatter(h, i).wait_recv()
                total = total + recv_ref[h, i].astype(F32)
            spec_ref[col, h] = total.astype(BF)
            for i in range(1, n_col):
                share(h, i).start()
        for h in range(halves):
            for i in range(1, n_col):
                share(h, i).wait_recv()
        for s in range(n_col):
            left, right = [], []
            for h in range(halves):
                spec = spec_ref[s, h].astype(F32)
                re, im = spec[:, :L // 2], spec[:, L // 2:]
                left.append(jnp.concatenate([re, re], axis=-1))
                right.append(jnp.concatenate([-im, im], axis=-1))
            for k in range(kyl):
                mixed = None
                for h in range(halves):
                    rows, chans = slice(k * CH, (k + 1) * CH), slice(h * CH, (h + 1) * CH)
                    term = left[h][rows][None] * wa_ref[k, :, chans]
                    term = term + right[h][rows][None] * wb_ref[k, :, chans]
                    mixed = term if mixed is None else mixed + term
                mix_ref[s, k * dl:(k + 1) * dl] = jnp.sum(mixed, axis=1).astype(BF)
        modes_ref[gx, gy, col] = mix_ref[col]

        def gather(i):
            px, py, pc = target((me + i) % N)
            return pltpu.make_async_remote_copy(
                src_ref=mix_ref.at[pc], dst_ref=modes_ref.at[gx, gy, col],
                send_sem=send3.at[i], recv_sem=recv3.at[i],
                device_id={"gx": px, "gy": py, "col": pc}, device_id_type=MESH,
            )

        loop(1, N, lambda i: gather(i).start())
        for h in range(halves):
            loop(1, nxy, lambda i: scatter(h, i).wait_send())
            for i in range(1, n_col):
                share(h, i).wait_send()
        loop(1, N, lambda i: gather(i).wait_recv())
        full = jnp.concatenate(
            [modes_ref[b].reshape(MY * C, L) for b in range(n_gx)], axis=-1
        )
        full = dot(cm_ref[...], full).astype(BF)
        for h in range(halves):
            part = full[h * MY * CH:(h + 1) * MY * CH]
            part = jnp.concatenate([dot(part, gx_ref[cs]).astype(BF) for cs in range(2)], axis=0)
            out_ref[:, h * CH:(h + 1) * CH] = dot(hy_ref[...], part).astype(BF).reshape(
                yl, CH, out_ref.shape[-1]
            )
        loop(1, N, lambda i: gather(i).wait_send())


def back_kernel(
    sizes, rows_ref, fields_ref, depth_ref, skip_ref, bias_ref, gain_ref, shift_ref, out_ref, wbd_ref
):
    G, C, MZ, Z, rows, tile = sizes

    @pl.when(pl.program_id(0) == 0)
    def _():
        weight = skip_ref[...].astype(F32)
        weight = (weight - jnp.mean(weight, axis=0, keepdims=True)).astype(BF)
        wbd_ref[...] = expand(
            weight, tile, tile,
            lambda i: mod(i, C), lambda j: mod(j, C), lambda i: div(i, C), lambda j: div(j, C),
        )

    def column(ref):
        return jnp.sum(jnp.where(iota((C, C), 0) == iota((C, C), 1), ref[...], 0.0), 1, keepdims=True)

    bias = column(bias_ref)
    bias = (bias - jnp.mean(bias, axis=0, keepdims=True))[None]
    gain = column(gain_ref)[None]
    shift = column(shift_ref)[None]
    for first in range(0, rows, tile):
        for x in range(0, G, 2):
            hidden = jnp.concatenate(
                [fields_ref[x + k, first:first + tile] for k in range(2)], axis=-1
            )
            pre = dot(wbd_ref[...], hidden) + dot(
                rows_ref[first:first + tile, x * 2 * MZ:(x + 2) * 2 * MZ], depth_ref[...]
            )
            pre = pre.reshape(tile // C, C, 2 * Z) + bias
            spread = jnp.mean(pre * pre, axis=1, keepdims=True)
            normed = pre * (lax.rsqrt(spread + norm_eps) * gain) + shift
            value = (0.5 * normed) * (1.0 + lax.erf(normed * (0.5 ** 0.5)))
            value = value.astype(BF).reshape(tile, 2 * Z)
            for k in range(2):
                out_ref[x + k, first:first + tile] = value[:, k * Z:(k + 1) * Z]


def build(mesh):
    n_gx, n_gy, n_col = (mesh.shape[a] for a in ("gx", "gy", "col"))

    def local(fields, spectral, skip_weight, skip_bias, norm_gain, norm_shift):
        hidden = fields[0]
        xl, yl, C, Z = hidden.shape
        weights = spectral[0]
        kxl, kyl, _, _, dl, MZ = weights.shape
        X, Y, MX, MY = xl * n_gx, yl * n_gy, kxl * n_gx, kyl * n_gy
        G = min(8, xl)
        steps = xl // G
        L = 2 * kxl * MZ
        N, nxy = n_gx * n_gy * n_col, n_gx * n_gy

        cz, sz = cos_sin(np.arange(Z), np.arange(MZ), Z)
        forward = np.concatenate([cz, -sz], axis=1)
        depth_forward = np.kron(np.eye(G), forward)
        backward = np.concatenate([cz.T, -sz.T], axis=0) / math.sqrt(MX * MY * MZ)
        depth_backward = np.kron(np.eye(2), backward)
        cy, sy = cos_sin(np.arange(Y), signed(MY), Y)
        tyf = np.stack([cy, sy]).reshape(2, n_gy, yl, MY).transpose(1, 0, 3, 2)
        tyf = tyf.reshape(n_gy, 2 * MY, yl)
        tyi = np.stack([cy, sy]).reshape(2, n_gy, yl, MY).transpose(1, 2, 0, 3)
        tyi = tyi.reshape(n_gy, yl, 2 * MY)
        cx, sx = cos_sin(np.arange(X), signed(MX), X)
        f = np.stack([
            np.stack([np.stack([cx, -sx], 1), np.stack([sx, cx], 1)], 1),
            np.stack([np.stack([-sx, -cx], 1), np.stack([cx, -sx], 1)], 1),
        ]) / math.sqrt(X * Y * Z)
        f = f.reshape(2, n_gx, steps, G, 2, 2, n_gx, kxl).transpose(1, 2, 0, 3, 4, 6, 5, 7)
        txf = f.reshape(n_gx, steps, 2, 2 * G, 2 * MX)
        b = np.stack([
            np.stack([np.stack([cx, sx]), np.stack([-sx, cx])]),
            np.stack([np.stack([-sx, cx]), np.stack([-cx, -sx])]),
        ])
        b = b.reshape(2, 2, 2, n_gx, xl, n_gx, kxl).transpose(3, 0, 5, 1, 6, 4, 2)
        txi = b.reshape(n_gx, 2, 2 * MX, 2 * xl)
        const = lambda a: jnp.asarray(a.astype(np.float32)).astype(BF)

        cells = hidden.reshape(xl, yl * C, Z)
        halves = 2 if C % 32 == 0 and n_col % 2 == 0 else 1
        CH = C // halves
        turned = jnp.transpose(weights, (0, 1, 2, 4, 5, 3))

        def whole(shape):
            return pl.BlockSpec(shape, lambda *_: (0,) * len(shape))

        sizes = (n_gx, n_gy, n_col, xl, yl, C, MY, MZ, kxl, kyl, dl, G, steps, halves)
        tables = [const(t) for t in (depth_forward, tyf, txf, txi, tyi)]
        rows_both = pl.pallas_call(
            functools.partial(front_kernel, sizes),
            grid=(halves, steps),
            out_shape=jax.ShapeDtypeStruct((yl, C, xl * 2 * MZ), BF),
            in_specs=[
                pl.BlockSpec((G, yl, CH, Z), lambda h, i: (i, 0, h, 0)),
                pl.BlockSpec(memory_space=pl.ANY),
            ] + [whole(t.shape) for t in tables],
            out_specs=whole((yl, C, xl * 2 * MZ)),
            scratch_shapes=[
                pltpu.VMEM((2 * MY * CH, yl * CH), BF),
                pltpu.VMEM((steps, 2, G * 2 * MZ, 2 * MX * MZ), BF),
                pltpu.VMEM((MY * CH, 2 * MX * MZ), F32),
                pltpu.VMEM((halves, n_gx, n_gy, kyl * CH, L), BF),
                pltpu.VMEM((halves, nxy, kyl * CH, L), BF),
                pltpu.VMEM((n_col, halves, kyl * CH, L), BF),
                pltpu.VMEM((n_col, kyl * dl, L), BF),
                pltpu.VMEM((n_gx, n_gy, n_col, kyl * dl, L), BF),
                pltpu.VMEM((2, 2 * MX * MZ, 2 * xl * MZ), BF),
                pltpu.VMEM((yl * CH, 2 * MY * CH), BF),
                pltpu.VMEM((MY * C, MY * C), BF),
                pltpu.VMEM(turned.shape, BF),
                pltpu.VMEM((kyl, dl, C, L), F32),
                pltpu.VMEM((kyl, dl, C, L), F32),
                pltpu.SemaphoreType.DMA,
                pltpu.SemaphoreType.DMA((halves, nxy)),
                pltpu.SemaphoreType.DMA((halves, nxy)),
                pltpu.SemaphoreType.DMA((halves, n_col)),
                pltpu.SemaphoreType.DMA((halves, n_col)),
                pltpu.SemaphoreType.DMA((N,)),
                pltpu.SemaphoreType.DMA((N,)),
            ],
            compiler_params=pltpu.CompilerParams(
                collective_id=0, has_side_effects=True, vmem_limit_bytes=34 * 2**20,
                dimension_semantics=("arbitrary", "arbitrary"),
            ),
            name="front",
        )(hidden, turned, *tables).reshape(yl * C, xl * 2 * MZ)

        G2 = min(4, xl)
        rows = yl * C
        tile = min(256, rows)
        out = pl.pallas_call(
            functools.partial(back_kernel, (G2, C, MZ, Z, rows, tile)),
            grid=(xl // G2,),
            out_shape=jax.ShapeDtypeStruct(cells.shape, BF),
            in_specs=[
                pl.BlockSpec((rows, G2 * 2 * MZ), lambda i: (0, i)),
                pl.BlockSpec((G2, rows, Z), lambda i: (i, 0, 0)),
                whole((4 * MZ, 2 * Z)), whole((C, C)), whole((1, C)), whole((1, C)), whole((1, C)),
            ],
            out_specs=pl.BlockSpec((G2, rows, Z), lambda i: (i, 0, 0)),
            scratch_shapes=[pltpu.VMEM((tile, tile), BF)],
            compiler_params=pltpu.CompilerParams(
                vmem_limit_bytes=20 * 2**20, dimension_semantics=("arbitrary",)
            ),
            name="back",
        )(
            rows_both, cells, const(depth_backward), skip_weight[0],
            skip_bias, norm_gain, norm_shift,
        )
        return out.reshape(1, xl, yl, C, Z)

    return local


def solution(mesh):
    placed = (
        P("col", "gx", "gy", None, None),
        P(None, "gx", "gy", None, None, "col", None),
        P(), P(), P(), P(),
    )
    return jax.shard_map(
        build(mesh), mesh=mesh, in_specs=placed,
        out_specs=P("col", "gx", "gy", None, None), check_vma=False,
    )
```

```python
import functools
import math

import jax
import jax.numpy as jnp
import numpy as np
from jax import lax
from jax.experimental import pallas as pl
from jax.experimental.pallas import tpu as pltpu
from jax.sharding import PartitionSpec as P

norm_eps = 1e-05
BF = jnp.bfloat16
F32 = jnp.float32
MESH = pl.DeviceIdType.MESH


def signed(count):
    index = np.arange(count)
    return np.where(index < count // 2, index, index - count)


def cos_sin(positions, frequency, length):
    turns = (positions[:, None] * frequency[None, :]) % length
    phase = turns * (2.0 * math.pi / length)
    return np.cos(phase), np.sin(phase)


def log2(n):
    assert n & (n - 1) == 0
    return n.bit_length() - 1


def div(i, n):
    return lax.shift_right_logical(i, jnp.int32(log2(n)))


def mod(i, n):
    return lax.bitwise_and(i, jnp.int32(n - 1))


def iota(shape, dim):
    return lax.broadcasted_iota(jnp.int32, shape, dim)


def dot(a, b):
    return jnp.dot(a, b, preferred_element_type=F32)


def expand(table, rows, cols, row_of, col_of, row_key, col_key, first_row=0):
    r, c = table.shape
    left = (row_of(iota((rows, r), 0) + first_row) == iota((rows, r), 1)).astype(F32).astype(BF)
    right = (col_of(iota((c, cols), 1)) == iota((c, cols), 0)).astype(F32).astype(BF)
    full = dot(dot(left, table).astype(BF), right)
    keep = row_key(iota((rows, cols), 0) + first_row) == col_key(iota((rows, cols), 1))
    return jnp.where(keep, full, 0.0).astype(BF)


def kron_eye(table, n, store, chunk=256):
    rows, cols = table.shape[0] * n, table.shape[1] * n
    chunk = min(chunk, rows)
    for first in range(0, rows, chunk):
        store(
            first,
            expand(
                table, chunk, cols,
                lambda i: div(i, n), lambda j: div(j, n),
                lambda i: mod(i, n), lambda j: mod(j, n), first,
            ),
        )


def front_kernel(
    sizes,
    fields_ref, spectral_ref, depth_ref, tyf_ref, txf_ref, txi_ref, tyi_ref,
    out_ref,
    ky_ref, kx_ref, total_ref, send_ref, recv_ref, spec_ref, mix_ref, modes_ref, gx_ref, hy_ref,
    cm_ref, w_ref, wa_ref, wb_ref,
    wsem, send1, recv1, send2, recv2, send3, recv3,
):
    n_gx, n_gy, n_col, xl, yl, C, MY, MZ, kxl, kyl, dl, G, steps, halves = sizes
    nxy, N = n_gx * n_gy, n_gx * n_gy * n_col
    L = 2 * kxl * MZ
    CH = C // halves
    per = n_col // halves
    half, step = pl.program_id(0), pl.program_id(1)
    gx, gy, col = lax.axis_index("gx"), lax.axis_index("gy"), lax.axis_index("col")

    unrolled = N <= 64
    at_gx = [lax.rem(gx + a, n_gx) for a in range(n_gx)] if unrolled else None
    at_gy = [lax.rem(gy + a, n_gy) for a in range(n_gy)] if unrolled else None
    at_col = [lax.rem(col + a, n_col) for a in range(n_col)] if unrolled else None

    def target(i):
        a, b, c = i // (n_gy * n_col), (i // n_col) % n_gy, i % n_col
        if unrolled:
            return at_gx[a], at_gy[b], at_col[c]
        return (gx + a) % n_gx, (gy + b) % n_gy, (col + c) % n_col

    def loop(low, high, body):
        if unrolled:
            for i in range(low, high):
                body(i)
            return

        def go(i, carry):
            body(i)
            return carry
        lax.fori_loop(low, high, go, 0)

    weights_copy = pltpu.make_async_copy(spectral_ref, w_ref, wsem)

    @pl.when((half == 0) & (step == 0))
    def _():
        barrier = pltpu.get_barrier_semaphore()

        def greet(i):
            px, py, pc = target(i)
            pl.semaphore_signal(
                barrier, inc=1, device_id={"gx": px, "gy": py, "col": pc}, device_id_type=MESH
            )

        loop(1, N, greet)
        weights_copy.start()

        def put(first, value):
            ky_ref[pl.ds(first, value.shape[0]), :] = value

        kron_eye(tyf_ref[gy], CH, put)

    @pl.when(half == 0)
    def _():
        for cs in range(2):
            def put(first, value, cs=cs):
                kx_ref[step, cs, pl.ds(first, value.shape[0]), :] = value
            kron_eye(txf_ref[gx, step, cs], MZ, put)

    lhs = jnp.concatenate(
        [fields_ref[g].reshape(yl * CH, fields_ref.shape[-1]) for g in range(G)], axis=-1
    )
    amplitude = dot(lhs, depth_ref[...]).astype(BF)
    turned = dot(ky_ref[...], amplitude).astype(BF)
    top = MY * CH
    term = dot(turned[:top], kx_ref[step, 0]) + dot(turned[top:], kx_ref[step, 1])

    @pl.when(step == 0)
    def _():
        total_ref[...] = term

    @pl.when(step > 0)
    def _():
        total_ref[...] += term

    def scatter(h, i):
        px, py, _ = target(i * n_col)
        return pltpu.make_async_remote_copy(
            src_ref=send_ref.at[h, px, py], dst_ref=recv_ref.at[h, i],
            send_sem=send1.at[h, i], recv_sem=recv1.at[h, i],
            device_id={"gx": px, "gy": py}, device_id_type=MESH,
        )

    @pl.when(step == steps - 1)
    def _():
        rows = kyl * CH
        for b in range(n_gx):
            block = total_ref[:, b * L:(b + 1) * L].astype(BF)
            for q in range(n_gy):
                send_ref[half, b, q] = block[q * rows:(q + 1) * rows]

        @pl.when(half == 0)
        def _():
            pl.semaphore_wait(pltpu.get_barrier_semaphore(), N - 1)

        loop(1, nxy, lambda i: scatter(half, i).start())

    @pl.when((half == halves - 1) & (step == steps - 1))
    def _():
        weights_copy.wait()
        eye = (iota((C, C), 0) == iota((C, C), 1)).astype(F32).astype(BF)
        turn = lambda a: lax.dot_general(
            eye, a, (((1,), (1,)), ((), ())), preferred_element_type=F32
        )
        for k in range(kyl):
            for d in range(dl):
                parts = [[w_ref[j, k, r, d] for j in range(kxl)] for r in range(2)]
                wa_ref[k, d] = turn(jnp.concatenate(parts[0] + parts[1], axis=0))
                wb_ref[k, d] = turn(jnp.concatenate(parts[1] + parts[0], axis=0))
        for cs in range(2):
            def put(first, value, cs=cs):
                gx_ref[cs, pl.ds(first, value.shape[0]), :] = value
            kron_eye(txi_ref[gx, cs], MZ, put)
        chunk = min(256, yl * CH)
        for first in range(0, yl * CH, chunk):
            hy_ref[pl.ds(first, chunk), :] = expand(
                tyi_ref[gy], chunk, 2 * MY * CH,
                lambda i: div(i, CH),
                lambda j: div(j, per * kyl * dl) * kyl + mod(div(j, dl), kyl),
                lambda i: mod(i, CH),
                lambda j: mod(div(j, kyl * dl), per) * dl + mod(j, dl),
                first,
            )
        shape = (MY * C, MY * C)
        i, j = iota(shape, 0), iota(shape, 1)
        in_half = mod(i, MY * CH)
        gy_i = div(in_half, per * kyl * dl)
        col_i = div(i, MY * CH) * per + mod(div(in_half, kyl * dl), per)
        source = (gy_i * n_col + col_i) * (kyl * dl) + mod(in_half, kyl * dl)
        same = (gy_i == div(j, n_col * kyl * dl)) & (mod(div(i, dl), kyl) == mod(div(j, dl), kyl))
        cm_ref[...] = (
            (source == j).astype(F32) - jnp.where(same, 1.0 / C, 0.0)
        ).astype(BF)

        def share(h, i):
            return pltpu.make_async_remote_copy(
                src_ref=spec_ref.at[col, h], dst_ref=spec_ref.at[col, h],
                send_sem=send2.at[h, i], recv_sem=recv2.at[h, i],
                device_id={"col": (col + i) % n_col}, device_id_type=MESH,
            )

        for h in range(halves):
            total = send_ref[h, gx, gy].astype(F32)
            for i in range(1, nxy):
                scatter(h, i).wait_recv()
                total = total + recv_ref[h, i].astype(F32)
            spec_ref[col, h] = total.astype(BF)
            for i in range(1, n_col):
                share(h, i).start()
        for h in range(halves):
            for i in range(1, n_col):
                share(h, i).wait_recv()
        for s in range(n_col):
            left, right = [], []
            for h in range(halves):
                spec = spec_ref[s, h].astype(F32)
                re, im = spec[:, :L // 2], spec[:, L // 2:]
                left.append(jnp.concatenate([re, re], axis=-1))
                right.append(jnp.concatenate([-im, im], axis=-1))
            for k in range(kyl):
                mixed = None
                for h in range(halves):
                    rows, chans = slice(k * CH, (k + 1) * CH), slice(h * CH, (h + 1) * CH)
                    term = left[h][rows][None] * wa_ref[k, :, chans]
                    term = term + right[h][rows][None] * wb_ref[k, :, chans]
                    mixed = term if mixed is None else mixed + term
                mix_ref[s, k * dl:(k + 1) * dl] = jnp.sum(mixed, axis=1).astype(BF)
        modes_ref[gx, gy, col] = mix_ref[col]

        def gather(i):
            px, py, pc = target(i)
            return pltpu.make_async_remote_copy(
                src_ref=mix_ref.at[pc], dst_ref=modes_ref.at[gx, gy, col],
                send_sem=send3.at[i], recv_sem=recv3.at[i],
                device_id={"gx": px, "gy": py, "col": pc}, device_id_type=MESH,
            )

        loop(1, N, lambda i: gather(i).start())
        for h in range(halves):
            loop(1, nxy, lambda i: scatter(h, i).wait_send())
            for i in range(1, n_col):
                share(h, i).wait_send()
        loop(1, N, lambda i: gather(i).wait_recv())
        full = jnp.concatenate(
            [modes_ref[b].reshape(MY * C, L) for b in range(n_gx)], axis=-1
        )
        full = dot(cm_ref[...], full).astype(BF)
        for h in range(halves):
            part = full[h * MY * CH:(h + 1) * MY * CH]
            part = jnp.concatenate([dot(part, gx_ref[cs]).astype(BF) for cs in range(2)], axis=0)
            out_ref[:, h * CH:(h + 1) * CH] = dot(hy_ref[...], part).astype(BF).reshape(
                yl, CH, out_ref.shape[-1]
            )
        loop(1, N, lambda i: gather(i).wait_send())


def back_kernel(
    sizes, rows_ref, fields_ref, depth_ref, skip_ref, bias_ref, gain_ref, shift_ref, out_ref, wbd_ref
):
    G, C, MZ, Z, rows, tile = sizes

    @pl.when(pl.program_id(0) == 0)
    def _():
        weight = skip_ref[...].astype(F32)
        weight = (weight - jnp.mean(weight, axis=0, keepdims=True)).astype(BF)
        wbd_ref[...] = expand(
            weight, tile, tile,
            lambda i: mod(i, C), lambda j: mod(j, C), lambda i: div(i, C), lambda j: div(j, C),
        )

    def column(ref):
        return jnp.sum(jnp.where(iota((C, C), 0) == iota((C, C), 1), ref[...], 0.0), 1, keepdims=True)

    bias = column(bias_ref)
    bias = (bias - jnp.mean(bias, axis=0, keepdims=True))[None]
    gain = column(gain_ref)[None]
    shift = column(shift_ref)[None]
    for first in range(0, rows, tile):
        for x in range(0, G, 2):
            hidden = jnp.concatenate(
                [fields_ref[x + k, first:first + tile] for k in range(2)], axis=-1
            )
            pre = dot(wbd_ref[...], hidden) + dot(
                rows_ref[first:first + tile, x * 2 * MZ:(x + 2) * 2 * MZ], depth_ref[...]
            )
            pre = pre.reshape(tile // C, C, 2 * Z) + bias
            spread = jnp.mean(pre * pre, axis=1, keepdims=True)
            normed = pre * (lax.rsqrt(spread + norm_eps) * gain) + shift
            value = (0.5 * normed) * (1.0 + lax.erf(normed * (0.5 ** 0.5)))
            value = value.astype(BF).reshape(tile, 2 * Z)
            for k in range(2):
                out_ref[x + k, first:first + tile] = value[:, k * Z:(k + 1) * Z]


def build(mesh):
    n_gx, n_gy, n_col = (mesh.shape[a] for a in ("gx", "gy", "col"))

    def local(fields, spectral, skip_weight, skip_bias, norm_gain, norm_shift):
        hidden = fields[0]
        xl, yl, C, Z = hidden.shape
        weights = spectral[0]
        kxl, kyl, _, _, dl, MZ = weights.shape
        X, Y, MX, MY = xl * n_gx, yl * n_gy, kxl * n_gx, kyl * n_gy
        G = min(8, xl)
        steps = xl // G
        L = 2 * kxl * MZ
        N, nxy = n_gx * n_gy * n_col, n_gx * n_gy

        cz, sz = cos_sin(np.arange(Z), np.arange(MZ), Z)
        forward = np.concatenate([cz, -sz], axis=1)
        depth_forward = np.kron(np.eye(G), forward)
        backward = np.concatenate([cz.T, -sz.T], axis=0) / math.sqrt(MX * MY * MZ)
        depth_backward = np.kron(np.eye(2), backward)
        cy, sy = cos_sin(np.arange(Y), signed(MY), Y)
        tyf = np.stack([cy, sy]).reshape(2, n_gy, yl, MY).transpose(1, 0, 3, 2)
        tyf = tyf.reshape(n_gy, 2 * MY, yl)
        tyi = np.stack([cy, sy]).reshape(2, n_gy, yl, MY).transpose(1, 2, 0, 3)
        tyi = tyi.reshape(n_gy, yl, 2 * MY)
        cx, sx = cos_sin(np.arange(X), signed(MX), X)
        f = np.stack([
            np.stack([np.stack([cx, -sx], 1), np.stack([sx, cx], 1)], 1),
            np.stack([np.stack([-sx, -cx], 1), np.stack([cx, -sx], 1)], 1),
        ]) / math.sqrt(X * Y * Z)
        f = f.reshape(2, n_gx, steps, G, 2, 2, n_gx, kxl).transpose(1, 2, 0, 3, 4, 6, 5, 7)
        txf = f.reshape(n_gx, steps, 2, 2 * G, 2 * MX)
        b = np.stack([
            np.stack([np.stack([cx, sx]), np.stack([-sx, cx])]),
            np.stack([np.stack([-sx, cx]), np.stack([-cx, -sx])]),
        ])
        b = b.reshape(2, 2, 2, n_gx, xl, n_gx, kxl).transpose(3, 0, 5, 1, 6, 4, 2)
        txi = b.reshape(n_gx, 2, 2 * MX, 2 * xl)
        const = lambda a: jnp.asarray(a.astype(np.float32)).astype(BF)

        cells = hidden.reshape(xl, yl * C, Z)
        halves = 2 if C % 32 == 0 and n_col % 2 == 0 else 1
        CH = C // halves
        turned = jnp.transpose(weights, (0, 1, 2, 4, 5, 3))

        def whole(shape):
            return pl.BlockSpec(shape, lambda *_: (0,) * len(shape))

        sizes = (n_gx, n_gy, n_col, xl, yl, C, MY, MZ, kxl, kyl, dl, G, steps, halves)
        tables = [const(t) for t in (depth_forward, tyf, txf, txi, tyi)]
        rows_both = pl.pallas_call(
            functools.partial(front_kernel, sizes),
            grid=(halves, steps),
            out_shape=jax.ShapeDtypeStruct((yl, C, xl * 2 * MZ), BF),
            in_specs=[
                pl.BlockSpec((G, yl, CH, Z), lambda h, i: (i, 0, h, 0)),
                pl.BlockSpec(memory_space=pl.ANY),
            ] + [whole(t.shape) for t in tables],
            out_specs=whole((yl, C, xl * 2 * MZ)),
            scratch_shapes=[
                pltpu.VMEM((2 * MY * CH, yl * CH), BF),
                pltpu.VMEM((steps, 2, G * 2 * MZ, 2 * MX * MZ), BF),
                pltpu.VMEM((MY * CH, 2 * MX * MZ), F32),
                pltpu.VMEM((halves, n_gx, n_gy, kyl * CH, L), BF),
                pltpu.VMEM((halves, nxy, kyl * CH, L), BF),
                pltpu.VMEM((n_col, halves, kyl * CH, L), BF),
                pltpu.VMEM((n_col, kyl * dl, L), BF),
                pltpu.VMEM((n_gx, n_gy, n_col, kyl * dl, L), BF),
                pltpu.VMEM((2, 2 * MX * MZ, 2 * xl * MZ), BF),
                pltpu.VMEM((yl * CH, 2 * MY * CH), BF),
                pltpu.VMEM((MY * C, MY * C), BF),
                pltpu.VMEM(turned.shape, BF),
                pltpu.VMEM((kyl, dl, C, L), F32),
                pltpu.VMEM((kyl, dl, C, L), F32),
                pltpu.SemaphoreType.DMA,
                pltpu.SemaphoreType.DMA((halves, nxy)),
                pltpu.SemaphoreType.DMA((halves, nxy)),
                pltpu.SemaphoreType.DMA((halves, n_col)),
                pltpu.SemaphoreType.DMA((halves, n_col)),
                pltpu.SemaphoreType.DMA((N,)),
                pltpu.SemaphoreType.DMA((N,)),
            ],
            compiler_params=pltpu.CompilerParams(
                collective_id=0, has_side_effects=True, vmem_limit_bytes=60 * 2**20,
                dimension_semantics=("arbitrary", "arbitrary"),
            ),
            name="front",
        )(hidden, turned, *tables).reshape(yl * C, xl * 2 * MZ)

        G2 = min(4, xl)
        rows = yl * C
        tile = min(256, rows)
        out = pl.pallas_call(
            functools.partial(back_kernel, (G2, C, MZ, Z, rows, tile)),
            grid=(xl // G2,),
            out_shape=jax.ShapeDtypeStruct(cells.shape, BF),
            in_specs=[
                pl.BlockSpec((rows, G2 * 2 * MZ), lambda i: (0, i)),
                pl.BlockSpec((G2, rows, Z), lambda i: (i, 0, 0)),
                whole((4 * MZ, 2 * Z)), whole((C, C)), whole((1, C)), whole((1, C)), whole((1, C)),
            ],
            out_specs=pl.BlockSpec((G2, rows, Z), lambda i: (i, 0, 0)),
            scratch_shapes=[pltpu.VMEM((tile, tile), BF)],
            compiler_params=pltpu.CompilerParams(
                vmem_limit_bytes=60 * 2**20, dimension_semantics=("arbitrary",)
            ),
            name="back",
        )(
            rows_both, cells, const(depth_backward), skip_weight[0],
            skip_bias, norm_gain, norm_shift,
        )
        return out.reshape(1, xl, yl, C, Z)

    return local


def solution(mesh):
    placed = (
        P("col", "gx", "gy", None, None),
        P(None, "gx", "gy", None, None, "col", None),
        P(), P(), P(), P(),
    )
    return jax.shard_map(
        build(mesh), mesh=mesh, in_specs=placed,
        out_specs=P("col", "gx", "gy", None, None), check_vma=False,
    )
```

```python
import functools
import math

import jax
import jax.numpy as jnp
import numpy as np
from jax import lax
from jax.experimental import pallas as pl
from jax.experimental.pallas import tpu as pltpu
from jax.sharding import PartitionSpec as P

norm_eps = 1e-05
BF = jnp.bfloat16
F32 = jnp.float32
MESH = pl.DeviceIdType.MESH


def signed(count):
    index = np.arange(count)
    return np.where(index < count // 2, index, index - count)


def cos_sin(positions, frequency, length):
    turns = (positions[:, None] * frequency[None, :]) % length
    phase = turns * (2.0 * math.pi / length)
    return np.cos(phase), np.sin(phase)


def log2(n):
    assert n & (n - 1) == 0
    return n.bit_length() - 1


def div(i, n):
    return lax.shift_right_logical(i, jnp.int32(log2(n)))


def mod(i, n):
    return lax.bitwise_and(i, jnp.int32(n - 1))


def iota(shape, dim):
    return lax.broadcasted_iota(jnp.int32, shape, dim)


def dot(a, b):
    return jnp.dot(a, b, preferred_element_type=F32)


def expand(table, rows, cols, row_of, col_of, row_key, col_key, first_row=0):
    r, c = table.shape
    left = (row_of(iota((rows, r), 0) + first_row) == iota((rows, r), 1)).astype(F32).astype(BF)
    right = (col_of(iota((c, cols), 1)) == iota((c, cols), 0)).astype(F32).astype(BF)
    full = dot(dot(left, table).astype(BF), right)
    keep = row_key(iota((rows, cols), 0) + first_row) == col_key(iota((rows, cols), 1))
    return jnp.where(keep, full, 0.0).astype(BF)


def kron_eye(table, n, store, chunk=256):
    rows, cols = table.shape[0] * n, table.shape[1] * n
    chunk = min(chunk, rows)
    for first in range(0, rows, chunk):
        store(
            first,
            expand(
                table, chunk, cols,
                lambda i: div(i, n), lambda j: div(j, n),
                lambda i: mod(i, n), lambda j: mod(j, n), first,
            ),
        )


def front_kernel(
    sizes,
    fields_ref, spectral_ref, depth_ref, tyf_ref, txf_ref, txi_ref, tyi_ref,
    out_ref,
    ky_ref, kx_ref, total_ref, send_ref, recv_ref, mix_ref, modes_ref, gx_ref, hy_ref,
    cm_ref, w_ref, wa_ref,
    wsem, send1, recv1, send2, recv2, send3, recv3,
):
    n_gx, n_gy, n_col, xl, yl, C, MY, MZ, kxl, kyl, dl, G, steps, halves = sizes
    nxy, N = n_gx * n_gy, n_gx * n_gy * n_col
    L = 2 * kxl * MZ
    CH = C // halves
    per = n_col // halves
    half, step = pl.program_id(0), pl.program_id(1)
    gx, gy, col = lax.axis_index("gx"), lax.axis_index("gy"), lax.axis_index("col")

    unrolled = N <= 64
    at_gx = [lax.rem(gx + a, n_gx) for a in range(n_gx)] if unrolled else None
    at_gy = [lax.rem(gy + a, n_gy) for a in range(n_gy)] if unrolled else None
    at_col = [lax.rem(col + a, n_col) for a in range(n_col)] if unrolled else None

    def target(i):
        a, b, c = i // (n_gy * n_col), (i // n_col) % n_gy, i % n_col
        if unrolled:
            return at_gx[a], at_gy[b], at_col[c]
        return (gx + a) % n_gx, (gy + b) % n_gy, (col + c) % n_col

    def loop(low, high, body):
        if unrolled:
            for i in range(low, high):
                body(i)
            return

        def go(i, carry):
            body(i)
            return carry
        lax.fori_loop(low, high, go, 0)

    weights_copy = pltpu.make_async_copy(spectral_ref, w_ref, wsem)

    @pl.when((half == 0) & (step == 0))
    def _():
        barrier = pltpu.get_barrier_semaphore()

        def greet(i):
            px, py, pc = target(i)
            pl.semaphore_signal(
                barrier, inc=1, device_id={"gx": px, "gy": py, "col": pc}, device_id_type=MESH
            )

        loop(1, nxy, lambda i: greet(i * n_col))
        loop(1, n_col, greet)
        weights_copy.start()

        def put(first, value):
            ky_ref[pl.ds(first, value.shape[0]), :] = value

        kron_eye(tyf_ref[gy], CH, put)

    @pl.when(half == 0)
    def _():
        for cs in range(2):
            def put(first, value, cs=cs):
                kx_ref[step, cs, pl.ds(first, value.shape[0]), :] = value
            kron_eye(txf_ref[gx, step, cs], MZ, put)

    lhs = jnp.concatenate(
        [fields_ref[g].reshape(yl * CH, fields_ref.shape[-1]) for g in range(G)], axis=-1
    )
    amplitude = dot(lhs, depth_ref[...]).astype(BF)
    turned = dot(ky_ref[...], amplitude).astype(BF)
    top = MY * CH
    term = dot(turned[:top], kx_ref[step, 0]) + dot(turned[top:], kx_ref[step, 1])

    @pl.when(step == 0)
    def _():
        total_ref[...] = term

    @pl.when(step > 0)
    def _():
        total_ref[...] += term

    def scatter(h, i):
        px, py, _ = target(i * n_col)
        return pltpu.make_async_remote_copy(
            src_ref=send_ref.at[h, px, py], dst_ref=recv_ref.at[h, i],
            send_sem=send1.at[h, i], recv_sem=recv1.at[h, i],
            device_id={"gx": px, "gy": py}, device_id_type=MESH,
        )

    def share(i):
        return pltpu.make_async_remote_copy(
            src_ref=wa_ref.at[col], dst_ref=wa_ref.at[col],
            send_sem=send2.at[i], recv_sem=recv2.at[i],
            device_id={"col": target(i)[2]}, device_id_type=MESH,
        )

    @pl.when((half == 0) & (step == min(1, steps - 1)))
    def _():
        weights_copy.wait()
        eye = (iota((C, C), 0) == iota((C, C), 1)).astype(F32).astype(BF)
        for k in range(kyl):
            for d in range(dl):
                parts = [w_ref[j, k, r, d] for r in range(2) for j in range(kxl)]
                wa_ref[col, k, d] = lax.dot_general(
                    eye, jnp.concatenate(parts, axis=0), (((1,), (1,)), ((), ())),
                    preferred_element_type=F32,
                ).astype(BF)
        pl.semaphore_wait(pltpu.get_barrier_semaphore(), nxy + n_col - 2)
        for i in range(1, n_col):
            share(i).start()

    @pl.when(step == steps - 1)
    def _():
        rows = kyl * CH
        for b in range(n_gx):
            block = total_ref[:, b * L:(b + 1) * L].astype(BF)
            for q in range(n_gy):
                send_ref[half, b, q] = block[q * rows:(q + 1) * rows]

        loop(1, nxy, lambda i: scatter(half, i).start())

    @pl.when((half == halves - 1) & (step == steps - 1))
    def _():
        for cs in range(2):
            def put(first, value, cs=cs):
                gx_ref[cs, pl.ds(first, value.shape[0]), :] = value
            kron_eye(txi_ref[gx, cs], MZ, put)
        chunk = min(256, yl * CH)
        for first in range(0, yl * CH, chunk):
            hy_ref[pl.ds(first, chunk), :] = expand(
                tyi_ref[gy], chunk, 2 * MY * CH,
                lambda i: div(i, CH),
                lambda j: div(j, per * kyl * dl) * kyl + mod(div(j, dl), kyl),
                lambda i: mod(i, CH),
                lambda j: mod(div(j, kyl * dl), per) * dl + mod(j, dl),
                first,
            )
        shape = (MY * C, MY * C)
        i, j = iota(shape, 0), iota(shape, 1)
        in_half = mod(i, MY * CH)
        gy_i = div(in_half, per * kyl * dl)
        col_i = div(i, MY * CH) * per + mod(div(in_half, kyl * dl), per)
        source = (gy_i * n_col + col_i) * (kyl * dl) + mod(in_half, kyl * dl)
        same = (gy_i == div(j, n_col * kyl * dl)) & (mod(div(i, dl), kyl) == mod(div(j, dl), kyl))
        cm_ref[...] = (
            (source == j).astype(F32) - jnp.where(same, 1.0 / C, 0.0)
        ).astype(BF)

        sums = {}
        for h in range(halves):
            total = send_ref[h, gx, gy].astype(F32)
            for i in range(1, nxy):
                scatter(h, i).wait_recv()
                total = total + recv_ref[h, i].astype(F32)
            spec = total.astype(BF).astype(F32)
            if h == 0:
                for i in range(1, n_col):
                    share(i).wait_recv()
            re, im = spec[:, :L // 2], spec[:, L // 2:]
            re = jnp.concatenate([re, re], axis=-1)
            im = jnp.concatenate([im, im], axis=-1)
            for q in range(n_col):
                for k in range(kyl):
                    rows, chans = slice(k * CH, (k + 1) * CH), slice(h * CH, (h + 1) * CH)
                    weight = wa_ref[q, k, :, chans].astype(F32)
                    new = [jnp.sum(v[rows][None] * weight, axis=1) for v in (re, im)]
                    old = sums.get((q, k))
                    sums[q, k] = new if old is None else [a + b for a, b in zip(old, new)]
        for q in range(n_col):
            for k in range(kyl):
                first, second = sums[q, k]
                turned_second = jnp.concatenate(
                    [-second[:, L // 2:], second[:, :L // 2]], axis=-1
                )
                row = (q * kyl + k) * dl
                mix_ref[row:row + dl] = (first + turned_second).astype(BF)
        modes_ref[gx, gy] = mix_ref[...]

        def gather(i):
            px, py, _ = target(i * n_col)
            return pltpu.make_async_remote_copy(
                src_ref=mix_ref, dst_ref=modes_ref.at[gx, gy],
                send_sem=send3.at[i], recv_sem=recv3.at[i],
                device_id={"gx": px, "gy": py}, device_id_type=MESH,
            )

        loop(1, nxy, lambda i: gather(i).start())
        for h in range(halves):
            loop(1, nxy, lambda i: scatter(h, i).wait_send())
        for i in range(1, n_col):
            share(i).wait_send()
        loop(1, nxy, lambda i: gather(i).wait_recv())
        full = jnp.concatenate(
            [modes_ref[b].reshape(MY * C, L) for b in range(n_gx)], axis=-1
        )
        full = dot(cm_ref[...], full).astype(BF)
        for h in range(halves):
            part = full[h * MY * CH:(h + 1) * MY * CH]
            part = jnp.concatenate([dot(part, gx_ref[cs]).astype(BF) for cs in range(2)], axis=0)
            out_ref[:, h * CH:(h + 1) * CH] = dot(hy_ref[...], part).astype(BF).reshape(
                yl, CH, out_ref.shape[-1]
            )
        loop(1, nxy, lambda i: gather(i).wait_send())


def back_kernel(
    sizes, rows_ref, fields_ref, depth_ref, skip_ref, bias_ref, gain_ref, shift_ref, out_ref, wbd_ref
):
    G, C, MZ, Z, rows, tile = sizes

    @pl.when(pl.program_id(0) == 0)
    def _():
        weight = skip_ref[...].astype(F32)
        weight = (weight - jnp.mean(weight, axis=0, keepdims=True)).astype(BF)
        wbd_ref[...] = expand(
            weight, tile, tile,
            lambda i: mod(i, C), lambda j: mod(j, C), lambda i: div(i, C), lambda j: div(j, C),
        )

    def column(ref):
        return jnp.sum(jnp.where(iota((C, C), 0) == iota((C, C), 1), ref[...], 0.0), 1, keepdims=True)

    bias = column(bias_ref)
    bias = (bias - jnp.mean(bias, axis=0, keepdims=True))[None]
    gain = column(gain_ref)[None]
    shift = column(shift_ref)[None]
    for first in range(0, rows, tile):
        for x in range(0, G, 2):
            hidden = jnp.concatenate(
                [fields_ref[x + k, first:first + tile] for k in range(2)], axis=-1
            )
            pre = dot(wbd_ref[...], hidden) + dot(
                rows_ref[first:first + tile, x * 2 * MZ:(x + 2) * 2 * MZ], depth_ref[...]
            )
            pre = pre.reshape(tile // C, C, 2 * Z) + bias
            spread = jnp.mean(pre * pre, axis=1, keepdims=True)
            normed = pre * (lax.rsqrt(spread + norm_eps) * gain) + shift
            value = (0.5 * normed) * (1.0 + lax.erf(normed * (0.5 ** 0.5)))
            value = value.astype(BF).reshape(tile, 2 * Z)
            for k in range(2):
                out_ref[x + k, first:first + tile] = value[:, k * Z:(k + 1) * Z]


def build(mesh):
    n_gx, n_gy, n_col = (mesh.shape[a] for a in ("gx", "gy", "col"))

    def local(fields, spectral, skip_weight, skip_bias, norm_gain, norm_shift):
        hidden = fields[0]
        xl, yl, C, Z = hidden.shape
        weights = spectral[0]
        kxl, kyl, _, _, dl, MZ = weights.shape
        X, Y, MX, MY = xl * n_gx, yl * n_gy, kxl * n_gx, kyl * n_gy
        G = min(8, xl)
        steps = xl // G
        L = 2 * kxl * MZ
        N, nxy = n_gx * n_gy * n_col, n_gx * n_gy

        cz, sz = cos_sin(np.arange(Z), np.arange(MZ), Z)
        forward = np.concatenate([cz, -sz], axis=1)
        depth_forward = np.kron(np.eye(G), forward)
        backward = np.concatenate([cz.T, -sz.T], axis=0) / math.sqrt(MX * MY * MZ)
        depth_backward = np.kron(np.eye(2), backward)
        cy, sy = cos_sin(np.arange(Y), signed(MY), Y)
        tyf = np.stack([cy, sy]).reshape(2, n_gy, yl, MY).transpose(1, 0, 3, 2)
        tyf = tyf.reshape(n_gy, 2 * MY, yl)
        tyi = np.stack([cy, sy]).reshape(2, n_gy, yl, MY).transpose(1, 2, 0, 3)
        tyi = tyi.reshape(n_gy, yl, 2 * MY)
        cx, sx = cos_sin(np.arange(X), signed(MX), X)
        f = np.stack([
            np.stack([np.stack([cx, -sx], 1), np.stack([sx, cx], 1)], 1),
            np.stack([np.stack([-sx, -cx], 1), np.stack([cx, -sx], 1)], 1),
        ]) / math.sqrt(X * Y * Z)
        f = f.reshape(2, n_gx, steps, G, 2, 2, n_gx, kxl).transpose(1, 2, 0, 3, 4, 6, 5, 7)
        txf = f.reshape(n_gx, steps, 2, 2 * G, 2 * MX)
        b = np.stack([
            np.stack([np.stack([cx, sx]), np.stack([-sx, cx])]),
            np.stack([np.stack([-sx, cx]), np.stack([-cx, -sx])]),
        ])
        b = b.reshape(2, 2, 2, n_gx, xl, n_gx, kxl).transpose(3, 0, 5, 1, 6, 4, 2)
        txi = b.reshape(n_gx, 2, 2 * MX, 2 * xl)
        const = lambda a: jnp.asarray(a.astype(np.float32)).astype(BF)

        cells = hidden.reshape(xl, yl * C, Z)
        halves = 2 if C % 32 == 0 and n_col % 2 == 0 else 1
        CH = C // halves
        turned = jnp.transpose(weights, (0, 1, 2, 4, 5, 3))

        def whole(shape):
            return pl.BlockSpec(shape, lambda *_: (0,) * len(shape))

        sizes = (n_gx, n_gy, n_col, xl, yl, C, MY, MZ, kxl, kyl, dl, G, steps, halves)
        tables = [const(t) for t in (depth_forward, tyf, txf, txi, tyi)]
        rows_both = pl.pallas_call(
            functools.partial(front_kernel, sizes),
            grid=(halves, steps),
            out_shape=jax.ShapeDtypeStruct((yl, C, xl * 2 * MZ), BF),
            in_specs=[
                pl.BlockSpec((G, yl, CH, Z), lambda h, i: (i, 0, h, 0)),
                pl.BlockSpec(memory_space=pl.ANY),
            ] + [whole(t.shape) for t in tables],
            out_specs=whole((yl, C, xl * 2 * MZ)),
            scratch_shapes=[
                pltpu.VMEM((2 * MY * CH, yl * CH), BF),
                pltpu.VMEM((steps, 2, G * 2 * MZ, 2 * MX * MZ), BF),
                pltpu.VMEM((MY * CH, 2 * MX * MZ), F32),
                pltpu.VMEM((halves, n_gx, n_gy, kyl * CH, L), BF),
                pltpu.VMEM((halves, nxy, kyl * CH, L), BF),
                pltpu.VMEM((kyl * C, L), BF),
                pltpu.VMEM((n_gx, n_gy, kyl * C, L), BF),
                pltpu.VMEM((2, 2 * MX * MZ, 2 * xl * MZ), BF),
                pltpu.VMEM((yl * CH, 2 * MY * CH), BF),
                pltpu.VMEM((MY * C, MY * C), BF),
                pltpu.VMEM(turned.shape, BF),
                pltpu.VMEM((n_col, kyl, dl, C, L), BF),
                pltpu.SemaphoreType.DMA,
                pltpu.SemaphoreType.DMA((halves, nxy)),
                pltpu.SemaphoreType.DMA((halves, nxy)),
                pltpu.SemaphoreType.DMA((n_col,)),
                pltpu.SemaphoreType.DMA((n_col,)),
                pltpu.SemaphoreType.DMA((nxy,)),
                pltpu.SemaphoreType.DMA((nxy,)),
            ],
            compiler_params=pltpu.CompilerParams(
                collective_id=0, has_side_effects=True, vmem_limit_bytes=60 * 2**20,
                dimension_semantics=("arbitrary", "arbitrary"),
            ),
            name="front",
        )(hidden, turned, *tables).reshape(yl * C, xl * 2 * MZ)

        G2 = min(4, xl)
        rows = yl * C
        tile = min(256, rows)
        out = pl.pallas_call(
            functools.partial(back_kernel, (G2, C, MZ, Z, rows, tile)),
            grid=(xl // G2,),
            out_shape=jax.ShapeDtypeStruct(cells.shape, BF),
            in_specs=[
                pl.BlockSpec((rows, G2 * 2 * MZ), lambda i: (0, i)),
                pl.BlockSpec((G2, rows, Z), lambda i: (i, 0, 0)),
                whole((4 * MZ, 2 * Z)), whole((C, C)), whole((1, C)), whole((1, C)), whole((1, C)),
            ],
            out_specs=pl.BlockSpec((G2, rows, Z), lambda i: (i, 0, 0)),
            scratch_shapes=[pltpu.VMEM((tile, tile), BF)],
            compiler_params=pltpu.CompilerParams(
                vmem_limit_bytes=60 * 2**20, dimension_semantics=("arbitrary",)
            ),
            name="back",
        )(
            rows_both, cells, const(depth_backward), skip_weight[0],
            skip_bias, norm_gain, norm_shift,
        )
        return out.reshape(1, xl, yl, C, Z)

    return local


def solution(mesh):
    placed = (
        P("col", "gx", "gy", None, None),
        P(None, "gx", "gy", None, None, "col", None),
        P(), P(), P(), P(),
    )
    return jax.shard_map(
        build(mesh), mesh=mesh, in_specs=placed,
        out_specs=P("col", "gx", "gy", None, None), check_vma=False,
    )
```
